32 devices in a mesh: row: 4 (over y, x), col: 8 (over z, core).
Axes of the slice: x: 2, y: 2, z: 4, core: 2. Of those that a mesh axis runs over, the one named last changes fastest.
Arguments:
- known_inverse: float32 [12288, 12288], P('col', 'row'), may hold values from -6 to 6
- factor_sep: float32 [12288, 1536], P('col'), may hold values from -0.09375 to 0.09375
- factor_pair: float32 [1536, 1536], P('col'), may hold values from -0.25 to 0.25
- pivot_inverse: float32 [1536, 1536], P('col', 'row'), may hold values from -6 to 6
- widths: int32 [8], replicated, may hold values from 1 to 512, 1536 in all
- parent_of: int32 [8], replicated, may hold values from -1 to 7, as said below
- ancestors: int32 [8, 24], replicated, may hold values from 0 to 63, all different within a row
Outputs:
- panel_inverse: float32 [1536, 12288], P('col', 'row')
- block_inverse: float32 [1536, 1536], P('col', 'row')
The draws below stay inside these ranges and needn't reach their ends.
Inputs may be any that keep to these rules, and one draw needn't show every extreme that they name: `parent_of`: exactly 4 supernodes have -1; each other one names one of those. `ancestors`: each supernode lists different blocks; every block is listed by some supernode. The widths sum to 1536.
All inputs are finite; a program needn't handle non-finite values.
Results may differ from the reference program's by a relative error of at most 0.0003.
Values sent between devices are 32-bit elements; how exact they have to be, the bound alone decides.
A program may use at most 192 MiB of HBM per device.

```python
import math
import jax
import jax.numpy as jnp
import numpy as np
from jax import lax

NS = 12288
WTOT = 1536
NSUP = 8
NUP = 4
NBLK = 64
ANC = 24
WMOST = 512


def draw_parent_of(key, part):
    order_key, pick_key = jax.random.split(jax.random.fold_in(key, 11))
    ordering = jax.random.permutation(order_key, NSUP).astype(jnp.int32)
    position = jnp.argsort(ordering).astype(jnp.int32)
    is_upper = position < NUP
    chosen = jax.random.randint(pick_key, (NSUP,), 0, NUP).astype(jnp.int32)
    parents = ordering[chosen]
    return jnp.where(is_upper, -1, parents).astype(jnp.int32)


def steps_of(own_key, extent, cuts, least, top_value):
    def one(dim, parts):
        draws = jax.random.uniform(jax.random.fold_in(jax.random.fold_in(own_key, 6), dim), (parts,), jnp.float32, least / len(cuts), top_value / len(cuts))
        return jnp.repeat(jnp.exp(draws), extent[dim] // parts).reshape((-1,) + (1,) * (len(extent) - dim - 1))

    gain = one(*cuts[0])
    for cut in cuts[1:]:
        gain = gain * one(*cut)
    return gain


def choose_distinct(key, rows, number_of, top, lift):
    ranking = jax.random.permutation(jax.random.fold_in(key, 1), number_of)
    boost = ranking
    for power in range(3):
        boost = boost * boost // number_of
    boost = boost * lift // number_of
    tickets = jax.random.randint(jax.random.fold_in(key, 2), (rows, number_of), 0, 4096) + boost
    holders = jax.random.permutation(jax.random.fold_in(key, 3), rows)[jnp.arange(number_of) % rows]
    tickets = jnp.where(jnp.arange(rows)[:, None] == holders[None, :], 1 << 14, tickets)
    score = tickets * number_of + jnp.arange(number_of)
    return lax.top_k(score.astype(jnp.int32), top)[1].astype(jnp.int32)


def split_up(amount, total, reach, lean):
    loads = [(1 << 20) // math.isqrt(standing ** lean) + 1 for standing in range(2, amount + 1)]
    surplus, holding = total - reach - (amount - 1), [1] * (amount - 1)
    while surplus > 0:
        free = [i for i in range(amount - 1) if holding[i] < reach]
        whole, budget = sum([loads[i] for i in free]), surplus
        for i in free:
            extra = min(reach - holding[i], max(1, budget * loads[i] // whole), surplus)
            holding[i] = holding[i] + extra
            surplus = surplus - extra
    return np.array([reach] + holding)


def uneven_parts(own_key, count, total, most, skew):
    if count == 2:
        one = jax.random.randint(own_key, (), max(1, total - most), min(most, total - 1) + 1)
        return jnp.stack([one, total - one])
    tallies = jnp.asarray(split_up(count, total, most, skew), jnp.int32)
    couples = (count - 1) // 2
    source_of, receiver = tallies[1:1 + 2 * couples:2], tallies[2:2 + 2 * couples:2]
    slack = jnp.minimum(source_of - 1, most - receiver)
    moved = jax.random.randint(jax.random.fold_in(own_key, 1), (couples,), 0, 1 << 20) % (slack + 1)
    tallies = tallies.at[1:1 + 2 * couples:2].set(source_of - moved).at[2:2 + 2 * couples:2].set(receiver + moved)
    return tallies[jax.random.permutation(jax.random.fold_in(own_key, 2), count)]


def centred(key, shape, spread, bound, pieces=(), held_as=jnp.bfloat16):
    entries = spread * jax.random.normal(key, shape, jnp.float32)
    if pieces:
        entries = entries * steps_of(key, shape, pieces, -0.22, 0.18)
    return jnp.clip(entries, -bound, bound).astype(held_as)


def setup_inputs(seed: int = 0) -> dict:
    arg_keys = jax.random.split(jax.random.key(seed), 8)
    known_inverse = centred(arg_keys[0], (NS, NS), 1.0, 6.0, ((0, 8), (1, 4)), jnp.float32)
    factor_sep = centred(arg_keys[1], (NS, WTOT), (NS * ANC // NBLK) ** -0.5, 0.09375, ((0, 8),), jnp.float32)
    factor_pair = centred(arg_keys[2], (WTOT, WTOT), WMOST ** -0.5, 0.25, ((0, 8),), jnp.float32)
    pivot_inverse = centred(arg_keys[3], (WTOT, WTOT), 1.0, 6.0, ((0, 8), (1, 4)), jnp.float32)
    widths = uneven_parts(arg_keys[4], NSUP, WTOT, WMOST, 2).astype(jnp.int32)
    parent_of = draw_parent_of(jax.random.fold_in(arg_keys[7], 71), 0)
    ancestors = choose_distinct(arg_keys[6], NSUP, NBLK, ANC, 6144)
    return {"known_inverse": known_inverse, "factor_sep": factor_sep, "factor_pair": factor_pair, "pivot_inverse": pivot_inverse, "widths": widths, "parent_of": parent_of, "ancestors": ancestors}


exact_mode = lax.Precision.HIGHEST


def plain_dot(left, right):
    return jnp.dot(left, right, precision=exact_mode, preferred_element_type=jnp.float32)


def first_dot(left, right):
    return lax.dot_general(left, right, (((0,), (0,)), ((), ())), precision=exact_mode, preferred_element_type=jnp.float32)


def supernode_tables(widths, parent_of, ancestors):
    position = jnp.arange(WTOT, dtype=jnp.int32)
    width_ends = jnp.cumsum(widths).astype(jnp.int32)
    column_owner = jnp.sum((width_ends[None, :] <= position[:, None]).astype(jnp.int32), axis=1).astype(jnp.int32)
    owner_onehot = column_owner[:, None] == jnp.arange(NSUP, dtype=jnp.int32)[None, :]
    listed = jnp.any(ancestors[:, :, None] == jnp.arange(NBLK, dtype=jnp.int32)[None, None, :], axis=1).astype(jnp.float32)
    column_blocks = plain_dot(owner_onehot.astype(jnp.float32), listed)
    column_parent = jnp.sum(jnp.where(owner_onehot, parent_of[None, :], 0), axis=1).astype(jnp.int32)
    column_upper = column_parent < 0
    return column_owner, column_blocks, column_parent, column_upper


def reference(known_inverse, factor_sep, factor_pair, pivot_inverse, widths, parent_of, ancestors):
    column_owner, column_blocks, column_parent, column_upper = supernode_tables(widths, parent_of, ancestors)
    sep_index = jnp.arange(NS, dtype=jnp.int32)
    block_onehot = ((sep_index // (NS // NBLK))[:, None] == jnp.arange(NBLK, dtype=jnp.int32)[None, :]).astype(jnp.float32)
    sep_factor = factor_sep * plain_dot(block_onehot, column_blocks.T)
    upper_cols = column_upper.astype(jnp.float32)
    lower_cols = 1.0 - upper_cols
    coupling = jnp.where((column_owner[:, None] == column_parent[None, :]) & (~column_upper)[None, :], factor_pair, 0.0)
    matching = column_owner[:, None] == column_owner[None, :]
    upper_factor = sep_factor * upper_cols[None, :]
    lower_factor = sep_factor * lower_cols[None, :]
    product = -first_dot(sep_factor, known_inverse)
    panel_upper = product * upper_cols[:, None]
    upper_block = jnp.where(matching & column_upper[None, :], pivot_inverse - plain_dot(panel_upper, upper_factor), 0.0)
    panel_lower = product * lower_cols[:, None] - first_dot(coupling, panel_upper)
    pair_block = jnp.where(column_owner[:, None] == column_parent[None, :], -(plain_dot(panel_upper, lower_factor) + plain_dot(upper_block, coupling)), 0.0)
    lower_block = jnp.where(matching & (~column_upper)[None, :], pivot_inverse - plain_dot(panel_lower, lower_factor) - first_dot(pair_block, coupling), 0.0)
    return panel_upper + panel_lower, upper_block + lower_block + pair_block
```

```python
import functools

import jax
import jax.numpy as jnp
from jax import lax
from jax.experimental import pallas as pl
from jax.experimental.pallas import tpu as pltpu
from jax.sharding import PartitionSpec as P

NS = 12288
WTOT = 1536
NSUP = 8
NBLK = 64

MESH = pl.DeviceIdType.MESH
exact_mode = lax.Precision.HIGH


def plain_dot(left, right):
    return jnp.dot(left, right, precision=exact_mode, preferred_element_type=jnp.float32)


def first_dot(left, right):
    return lax.dot_general(
        left,
        right,
        (((0,), (0,)), ((), ())),
        precision=exact_mode,
        preferred_element_type=jnp.float32,
    )

def supernode_tables(widths, parent_of, ancestors):
    position = jnp.arange(WTOT, dtype=jnp.int32)
    width_ends = jnp.cumsum(widths)
    column_owner = jnp.sum((width_ends[None, :] <= position[:, None]).astype(jnp.int32), axis=1)
    owner_onehot = column_owner[:, None] == jnp.arange(NSUP, dtype=jnp.int32)[None, :]
    listed = jnp.any(
        ancestors[:, :, None] == jnp.arange(NBLK, dtype=jnp.int32)[None, None, :], axis=1
    ).astype(jnp.float32)
    column_blocks = plain_dot(owner_onehot.astype(jnp.float32), listed)
    column_parent = jnp.sum(jnp.where(owner_onehot, parent_of[None, :], 0), axis=1)
    column_upper = column_parent < 0
    return (column_owner, column_blocks, column_parent, column_upper)


def line_kernel(chunks, chips, width, deal, *refs):
    if deal:
        high, low, known, panel, dealt, own, pair, below, above, sems, *refs = refs
        deal_send, deal_recv, fetched, known_high, known_low, sent, fetch = refs
    else:
        part, panel, own, pair, below, above, sems = refs
    load, pair_send, pair_recv, up_send, up_recv, down_send, down_recv, store = (
        sems.at[i] for i in range(8)
    )
    row = lax.axis_index("row")
    col = lax.axis_index("col")
    chip = col // 2
    core = col % 2
    other = col + 1 - 2 * core
    last = chips - 1
    half = max(chunks // 2, 1)
    lag = 2 if deal else 0
    depth = panel.shape[0]

    barrier = pltpu.get_barrier_semaphore()

    def greet(device):
        pl.semaphore_signal(barrier, inc=1, device_id=device, device_id_type=MESH)

    greet((row, other))

    @pl.when(chip > 0)
    def _():
        greet((row, col - 2))

    @pl.when(chip < last)
    def _():
        greet((row, col + 2))

    met = 1 + (chip > 0).astype(jnp.int32) + (chip < last).astype(jnp.int32)
    if deal:

        @pl.when(chip != row)
        def _():
            greet((chip, 2 * row))
            greet((chip, 2 * row + 1))

        met = met + 2 * (chip != row).astype(jnp.int32)
    pl.semaphore_wait(barrier, met)

    def span(j):
        if chunks == 1:
            return pl.ds(0, width)
        return pl.ds(pl.multiple_of(j * width, width), width)

    def load_copy(j):
        return pltpu.make_async_copy(part.at[:, core, :, span(j)], own.at[j], load.at[j])

    def remote(src, dst, send, recv, device):
        return pltpu.make_async_remote_copy(
            src_ref=src, dst_ref=dst, send_sem=send, recv_sem=recv,
            device_id=device, device_id_type=MESH,
        )

    def pair_copy(j):
        source = sent.at[j % 4] if deal else part.at[:, 1 - core, :, span(j)]
        return remote(source, pair.at[j], pair_send.at[j], pair_recv.at[j], (row, other))

    def fetch_copy(g):
        columns = pl.ds(pl.multiple_of(2 * g * width, 2 * width), 2 * width)
        return pltpu.make_async_copy(known.at[:, columns], fetched.at[g % 2], fetch.at[g % 2])

    def up_copy(j, at):
        units = pl.ds(at + 1, last - at)
        return remote(own.at[j, units], below.at[j, units], up_send.at[j], up_recv.at[j], (row, col + 2))

    def down_copy(j, at):
        units = pl.ds(0, at)
        return remote(own.at[j, units], above.at[j, units], down_send.at[j], down_recv.at[j], (row, col - 2))

    def store_copy(j):
        return pltpu.make_async_copy(own.at[j, chip], panel.at[:, span(j)], store.at[j])

    def kept(j):
        return (chip == row) & (j // half == core)

    def deal_spot(j):
        return dealt.at[core, :, span(j % half)]

    def deal_copy(j):
        return remote(
            own.at[j, chip], deal_spot(j), deal_send.at[j], deal_recv.at[core, j % half],
            (chip, 2 * row + j // half),
        )

    def keep_copy(j):
        return pltpu.make_async_copy(own.at[j, chip], deal_spot(j), deal_recv.at[core, j % half])

    def begin(j, carry):
        load_copy(j).start()
        pair_copy(j).start()
        return carry

    if deal:
        fetch_copy(0).start()
    else:
        lax.fori_loop(0, chunks, begin, 0)

    def multiply(t):
        g = t // 2
        fetch_copy(g).wait()

        @pl.when(g + 1 < half)
        def _():
            fetch_copy(g + 1).start()

        @pl.when(t >= 4)
        def _():
            pair_copy(t - 4).wait_send()
            pair_copy(t - 3).wait_send()

        def split(i, carry):
            at = pl.ds(pl.multiple_of(i * 2 * width, 2 * width), 2 * width)
            block = fetched[g % 2, at, :]
            rounded = block.astype(jnp.bfloat16)
            known_high[at, :] = rounded
            known_low[at, :] = (block - rounded.astype(jnp.float32)).astype(jnp.bfloat16)
            return carry

        lax.fori_loop(0, fetched.shape[1] // (2 * width), split, 0)

        def unit(d, carry):
            at = pl.ds(pl.multiple_of(d * 2 * depth, 2 * depth), 2 * depth)
            total = jnp.dot(high[at, :], known_low[...], preferred_element_type=jnp.float32)
            total += jnp.dot(low[at, :], known_high[...], preferred_element_type=jnp.float32)
            total += jnp.dot(high[at, :], known_high[...], preferred_element_type=jnp.float32)
            for side in range(2):

                @pl.when(core == side)
                def _():
                    for i in range(2):
                        piece = total[:, i * width : (i + 1) * width]
                        own[t + i, d] = piece[side * depth : (side + 1) * depth]
                        sent[(t + i) % 4, d] = piece[(1 - side) * depth : (2 - side) * depth]

            return carry

        lax.fori_loop(0, chips, unit, 0)

    def tick(t, carry):
        if deal:

            @pl.when((t < chunks) & (t % 2 == 0))
            def _():
                multiply(t)

        sum_at = t - lag

        @pl.when((sum_at >= 0) & (sum_at < chunks))
        def _():
            if not deal:
                load_copy(sum_at).wait()
            pair_copy(sum_at).wait_recv()
            own[sum_at] = own[sum_at] + pair[sum_at]

        if deal:

            @pl.when((t < chunks) & (t % 2 == 0))
            def _():
                pair_copy(t).start()
                pair_copy(t + 1).start()

        up = sum_at - chip
        down = sum_at - (last - chip)
        ready = sum_at - jnp.maximum(chip, last - chip)
        for at in range(chips):

            @pl.when((chip == at) & (up >= 0) & (up < chunks))
            def _():
                if at > 0:
                    up_copy(up, at - 1).wait_recv()
                    for d in range(at, chips):
                        own[up, d] = own[up, d] + below[up, d]

            @pl.when((chip == at) & (down >= 0) & (down < chunks))
            def _():
                if at < last:
                    down_copy(down, at + 1).wait_recv()
                    for d in range(at + 1):
                        own[down, d] = own[down, d] + above[down, d]

            @pl.when((chip == at) & (up >= 0) & (up < chunks))
            def _():
                if at < last:
                    up_copy(up, at).start()

            @pl.when((chip == at) & (down >= 0) & (down < chunks))
            def _():
                if at > 0:
                    down_copy(down, at).start()

        @pl.when((ready >= 0) & (ready < chunks))
        def _():
            store_copy(ready).start()
            if deal:

                @pl.when(kept(ready))
                def _():
                    keep_copy(ready).start()

                @pl.when(jnp.logical_not(kept(ready)))
                def _():
                    deal_copy(ready).start()

        return carry

    lax.fori_loop(0, chunks + last + lag, tick, 0)

    def finish(j, carry):
        @pl.when(j >= (chunks - 4 if deal else 0))
        def _():
            pair_copy(j).wait_send()

        store_copy(j).wait()
        for at in range(chips):

            @pl.when(chip == at)
            def _():
                if at < last:
                    up_copy(j, at).wait_send()
                if at > 0:
                    down_copy(j, at).wait_send()

        if deal:

            @pl.when(jnp.logical_not(kept(j)))
            def _():
                deal_copy(j).wait_send()

        return carry

    lax.fori_loop(0, chunks, finish, 0)
    if deal:

        def landed(i, carry):
            spot = dealt.at[i // half, :, span(i % half)]
            pltpu.make_async_copy(own.at[0, 0], spot, deal_recv.at[i // half, i % half]).wait()
            return carry

        lax.fori_loop(0, 2 * half, landed, 0)


ANYWHERE = pl.BlockSpec(memory_space=pl.ANY)


def line_params(number):
    return pltpu.CompilerParams(
        collective_id=number, has_side_effects=True, vmem_limit_bytes=62 << 20
    )


def line_scratch(chunks, chips, depth, width):
    block = pltpu.VMEM((chunks, chips, depth, width), jnp.float32)
    return [block] * 4 + [pltpu.SemaphoreType.DMA((8, chunks))]


def panel_reduce(high, low, known, chips, depth):
    inner, wide = known.shape
    width = 128
    chunks = wide // width
    return pl.pallas_call(
        functools.partial(line_kernel, chunks, chips, width, True),
        out_shape=[
            jax.ShapeDtypeStruct((depth, wide), jnp.float32),
            jax.ShapeDtypeStruct((2, depth, wide // 2), jnp.float32),
        ],
        in_specs=[pl.BlockSpec(memory_space=pltpu.VMEM)] * 2 + [ANYWHERE],
        out_specs=[ANYWHERE] * 2,
        scratch_shapes=line_scratch(chunks, chips, depth, width)
        + [
            pltpu.SemaphoreType.DMA((chunks,)),
            pltpu.SemaphoreType.DMA((2, chunks // 2)),
            pltpu.VMEM((2, inner, 2 * width), jnp.float32),
            pltpu.VMEM((inner, 2 * width), jnp.bfloat16),
            pltpu.VMEM((inner, 2 * width), jnp.bfloat16),
            pltpu.VMEM((4, chips, depth, width), jnp.float32),
            pltpu.SemaphoreType.DMA((2,)),
        ],
        compiler_params=line_params(1),
        name="panel_reduce",
    )(high, low, known)


def block_reduce(part):
    chips, _, depth, wide = part.shape
    chunks = wide // 128 if wide % 128 == 0 else 1
    return pl.pallas_call(
        functools.partial(line_kernel, chunks, chips, wide // chunks, False),
        out_shape=jax.ShapeDtypeStruct((depth, wide), jnp.float32),
        in_specs=[ANYWHERE],
        out_specs=ANYWHERE,
        scratch_shapes=line_scratch(chunks, chips, depth, wide // chunks),
        compiler_params=line_params(2),
        name="block_reduce",
    )(part)


def plane_kernel(rows, part, total, arrived, sends, recvs):
    row = lax.axis_index("row")
    col = lax.axis_index("col")
    tall = total.shape[1]
    barrier = pltpu.get_barrier_semaphore()
    for step in range(1, rows):
        device = (lax.rem(row + step, rows), col)
        pl.semaphore_signal(barrier, inc=1, device_id=device, device_id_type=MESH)
    pl.semaphore_wait(barrier, rows - 1)

    def copy(step):
        target = lax.rem(row + step, rows)
        columns = pl.ds(pl.multiple_of(target * tall, tall), tall)
        return pltpu.make_async_remote_copy(
            src_ref=part.at[:, columns], dst_ref=arrived.at[step],
            send_sem=sends.at[step], recv_sem=recvs.at[step],
            device_id=(target, col), device_id_type=MESH,
        )

    for step in range(1, rows):
        copy(step).start()
    columns = pl.ds(pl.multiple_of(row * tall, tall), tall)
    mine = pltpu.make_async_copy(part.at[:, columns], arrived.at[0], recvs.at[0])
    mine.start()
    mine.wait()
    for step in range(1, rows):
        copy(step).wait()
    result = arrived[0]
    for step in range(1, rows):
        result = result + arrived[step]
    total[...] = result


def plane_reduce(part, rows):
    depth, wide = part.shape
    tall = wide // rows
    if tall % 128:
        return lax.psum_scatter(part, "row", scatter_dimension=1, tiled=True)
    return pl.pallas_call(
        functools.partial(plane_kernel, rows),
        out_shape=jax.ShapeDtypeStruct((depth, tall), jnp.float32),
        in_specs=[ANYWHERE],
        out_specs=pl.BlockSpec(memory_space=pltpu.VMEM),
        scratch_shapes=[
            pltpu.VMEM((rows, depth, tall), jnp.float32),
            pltpu.SemaphoreType.DMA((rows,)),
            pltpu.SemaphoreType.DMA((rows,)),
        ],
        compiler_params=line_params(3),
        name="plane_reduce",
    )(part)


def gather_kernel(chips, mine, out, held, sems, stores):
    row = lax.axis_index("row")
    col = lax.axis_index("col")
    chip = col // 2
    core = col % 2
    other = col + 1 - 2 * core
    last = chips - 1
    piece = held.shape[2]
    along_x, along_y, across = row + 1 - 2 * (row % 2), (row + 2) % 4, 3 - row

    barrier = pltpu.get_barrier_semaphore()

    def greet(device):
        pl.semaphore_signal(barrier, inc=1, device_id=device, device_id_type=MESH)

    greet((row, other))
    greet((along_x, col))
    greet((along_y, col))

    @pl.when(chip > 0)
    def _():
        greet((row, col - 2))

    @pl.when(chip < last)
    def _():
        greet((row, col + 2))

    met = 3 + (chip > 0).astype(jnp.int32) + (chip < last).astype(jnp.int32)
    pl.semaphore_wait(barrier, met)

    def remote(ref, send, recv, spot, device):
        return pltpu.make_async_remote_copy(
            src_ref=ref, dst_ref=ref, send_sem=sems.at[send, spot], recv_sem=sems.at[recv, spot],
            device_id=device, device_id_type=MESH,
        )

    def item(at, quarter):
        return held.at[2 * at + core, quarter]

    def up(at):
        return remote(item(at, row), 0, 2, at, (row, col + 2))

    def down(at):
        return remote(item(at, row), 1, 2, at, (row, col - 2))

    def sideways_x(at):
        return remote(item(at, row), 3, 4, at, (along_x, col))

    def sideways_y(at):
        return remote(item(at, row), 5, 6, at, (along_y, col))

    def onward_x(at):
        return remote(item(at, along_y).at[pl.ds(0, piece // 2)], 7, 8, at, (along_x, col))

    def onward_y(at):
        return remote(
            item(at, along_x).at[pl.ds(piece // 2, piece // 2)], 9, 10, at, (along_y, col)
        )

    def hand(at, quarter):
        return remote(item(at, quarter), 11 + quarter, 15 + quarter, at, (row, other))

    def hand_own():
        return remote(held.at[col], 19, 20, 0, (row, other))

    def keep(c):
        return pltpu.make_async_copy(held.at[c], out.at[c], stores.at[c])

    def both_ways(visit):
        for distance in range(1, chips):

            @pl.when(chip - distance >= 0)
            def _():
                visit(chip - distance, True)

            @pl.when(chip + distance <= last)
            def _():
                visit(chip + distance, False)

    load = pltpu.make_async_copy(mine, held.at[col], sems.at[21, 0])
    load.start()
    load.wait()

    @pl.when(chip < last)
    def _():
        up(chip).start()

    @pl.when(chip > 0)
    def _():
        down(chip).start()

    hand_own().start()
    keep(col).start()

    def from_line(at, rising):
        if rising:
            up(at).wait_recv()

            @pl.when(chip < last)
            def _():
                up(at).start()

        else:
            down(at).wait_recv()

            @pl.when(chip > 0)
            def _():
                down(at).start()

        sideways_x(at).start()
        sideways_y(at).start()
        hand(at, row).start()

    def from_sides(at, rising):
        sideways_x(at).wait_recv()
        onward_y(at).start()
        hand(at, along_x).start()
        sideways_y(at).wait_recv()
        onward_x(at).start()
        hand(at, along_y).start()

    def from_across(at, rising):
        onward_x(at).wait_recv()
        onward_y(at).wait_recv()
        hand(at, across).start()
        keep(2 * at + core).start()

    def from_other(at, rising):
        for quarter in range(4):
            hand(at, quarter).wait_recv()
        keep(2 * at + 1 - core).start()

    both_ways(from_line)
    both_ways(from_sides)
    both_ways(from_across)
    hand_own().wait_recv()
    keep(other).start()
    both_ways(from_other)

    def drain(at, rising):
        if rising:

            @pl.when(chip < last)
            def _():
                up(at).wait_send()

        else:

            @pl.when(chip > 0)
            def _():
                down(at).wait_send()

        for copy in (sideways_x, sideways_y, onward_x, onward_y):
            copy(at).wait_send()
        for quarter in range(4):
            hand(at, quarter).wait_send()

    both_ways(drain)

    @pl.when(chip < last)
    def _():
        up(chip).wait_send()

    @pl.when(chip > 0)
    def _():
        down(chip).wait_send()

    hand_own().wait_send()
    for c in range(2 * chips):
        keep(c).wait()


def gather_rows(mine, rows, cols):
    depth, wide = mine.shape
    piece = depth // 4
    if rows != 4 or piece % 16:
        return lax.all_gather(mine, "col", axis=0, tiled=True)
    shape = (cols, 4, piece, wide)
    out = pl.pallas_call(
        functools.partial(gather_kernel, cols // 2),
        out_shape=jax.ShapeDtypeStruct(shape, jnp.float32),
        in_specs=[ANYWHERE],
        out_specs=ANYWHERE,
        scratch_shapes=[
            pltpu.VMEM(shape, jnp.float32),
            pltpu.SemaphoreType.DMA((22, cols // 2)),
            pltpu.SemaphoreType.DMA((cols,)),
        ],
        compiler_params=line_params(4),
        name="gather_rows",
    )(mine.reshape(4, piece, wide))
    return out.reshape(cols * depth, wide)


def shards(known_inverse, factor_sep, factor_pair, pivot_inverse, widths, parent_of, ancestors):
    col_index = lax.axis_index("col")
    row_index = lax.axis_index("row")
    rows = lax.axis_size("row")
    cols = lax.axis_size("col")
    chips = cols // 2
    chip, core = col_index // 2, col_index % 2
    sep_local = factor_sep.shape[0]
    pair_local = factor_pair.shape[0]
    wide_local = pivot_inverse.shape[1]
    column_owner, column_blocks, column_parent, column_upper = supernode_tables(
        widths, parent_of, ancestors
    )

    def rows_of(x, index, size):
        return lax.dynamic_slice_in_dim(x, index * size, size)

    def cols_of(x, index, size):
        return lax.dynamic_slice_in_dim(x, index * size, size, 1)

    sep_index = col_index * sep_local + jnp.arange(sep_local, dtype=jnp.int32)
    block_onehot = (
        (sep_index // (NS // NBLK))[:, None] == jnp.arange(NBLK, dtype=jnp.int32)[None, :]
    ).astype(jnp.float32)
    sep_factor = factor_sep * plain_dot(block_onehot, column_blocks.T)
    upper_cols = column_upper.astype(jnp.float32)
    owner_rows = rows_of(column_owner, col_index, pair_local)
    owner_wide = rows_of(column_owner, row_index, wide_local)
    parent_wide = rows_of(column_parent, row_index, wide_local)
    upper_wide = rows_of(column_upper, row_index, wide_local)
    coupling = jnp.where(
        (owner_rows[:, None] == column_parent[None, :]) & (~column_upper)[None, :], factor_pair, 0.0
    )
    matching = owner_rows[:, None] == owner_wide[None, :]
    match_pair = owner_rows[:, None] == parent_wide[None, :]

    coupling_all = gather_rows(coupling, rows, cols)

    straight = [
        (r * cols + 2 * z + q, z * cols + 2 * r + q)
        for r in range(rows)
        for z in range(chips)
        for q in range(2)
    ]
    crossed = [(source, target ^ 1) for source, target in straight]
    swapped = [(device, device ^ 1) for device in range(rows * cols)]

    def permute(x, order):
        return lax.ppermute(x, ("row", "col"), order)

    def ordered(mine, others):
        return jnp.where(
            core == 0, jnp.concatenate([mine, others]), jnp.concatenate([others, mine])
        )

    upper_pivot = jnp.where(matching & upper_wide[None, :], pivot_inverse, 0.0)
    pivot_tile = ordered(
        permute(cols_of(upper_pivot, core, pair_local), straight),
        permute(cols_of(upper_pivot, 1 - core, pair_local), crossed),
    )
    pivot_coupled = plain_dot(pivot_tile, coupling)

    lead = plain_dot(sep_factor * upper_cols[None, :], coupling_all) - sep_factor
    turned = lead.T
    high = lax.reduce_precision(turned, 8, 7)
    low = (turned - high).astype(jnp.bfloat16)
    panel, dealt = panel_reduce(
        high.astype(jnp.bfloat16), low, known_inverse, chips, pair_local
    )
    moved = dealt.reshape(wide_local, sep_local)

    moved_upper = jnp.where(upper_wide[:, None], moved, 0.0)
    moved_lower = jnp.where(upper_wide[:, None], 0.0, moved)
    product = plain_dot(moved_lower, sep_factor) - plain_dot(moved_upper, lead) + pivot_coupled
    product = product.reshape(2, pair_local, chips, wide_local).transpose(2, 0, 1, 3)
    tile = block_reduce(product)

    dealt_tile = permute(tile, straight)
    pair_tile = jnp.where(
        rows_of(column_owner, 2 * row_index + core, pair_local)[:, None]
        == rows_of(column_parent, chip, wide_local)[None, :],
        -tile,
        0.0,
    )
    pair_cols = ordered(
        cols_of(pair_tile, core, pair_local),
        permute(cols_of(pair_tile, 1 - core, pair_local), swapped),
    )
    below = first_dot(pair_cols, rows_of(coupling_all, row_index, wide_local))
    below = plane_reduce(below, rows)

    own_block = jnp.where(
        matching, pivot_inverse - dealt_tile - jnp.where(upper_wide[None, :], 0.0, below), 0.0
    )
    return panel, own_block + jnp.where(match_pair, -dealt_tile, 0.0)


def solution(mesh):
    if mesh.shape["col"] != 2 * mesh.shape["row"]:
        raise ValueError("unsupported mesh")
    in_specs = (P("col", "row"), P("col", None), P("col", None), P("col", "row"), P(), P(), P())
    out_specs = (P("col", "row"), P("col", "row"))
    return jax.shard_map(shards, mesh=mesh, in_specs=in_specs, out_specs=out_specs, check_vma=False)
```

```python
import functools

import jax
import jax.numpy as jnp
from jax import lax
from jax.experimental import pallas as pl
from jax.experimental.pallas import tpu as pltpu
from jax.sharding import PartitionSpec as P

NS = 12288
WTOT = 1536
NSUP = 8
NBLK = 64

MESH = pl.DeviceIdType.MESH
exact_mode = lax.Precision.HIGH


def plain_dot(left, right):
    return jnp.dot(left, right, precision=exact_mode, preferred_element_type=jnp.float32)


def first_dot(left, right):
    return lax.dot_general(
        left,
        right,
        (((0,), (0,)), ((), ())),
        precision=exact_mode,
        preferred_element_type=jnp.float32,
    )

def supernode_tables(widths, parent_of, ancestors):
    position = jnp.arange(WTOT, dtype=jnp.int32)
    width_ends = jnp.cumsum(widths)
    column_owner = jnp.sum((width_ends[None, :] <= position[:, None]).astype(jnp.int32), axis=1)
    owner_onehot = column_owner[:, None] == jnp.arange(NSUP, dtype=jnp.int32)[None, :]
    listed = jnp.any(
        ancestors[:, :, None] == jnp.arange(NBLK, dtype=jnp.int32)[None, None, :], axis=1
    ).astype(jnp.float32)
    column_blocks = plain_dot(owner_onehot.astype(jnp.float32), listed)
    column_parent = jnp.sum(jnp.where(owner_onehot, parent_of[None, :], 0), axis=1)
    column_upper = column_parent < 0
    return (column_owner, column_blocks, column_parent, column_upper)


def line_kernel(chunks, chips, width, deal, *refs):
    if deal:
        high, low, known, sep, lead, start, upper, panel, product, *refs = refs
        own, pair, below, above, sems, *refs = refs
        deal_send, deal_recv, fetched, known_high, known_low, sent, fetch, *refs = refs
        dealt, factors, total, factor_sems, total_sem = refs
    else:
        part, panel, own, pair, below, above, sems = refs
    load, pair_send, pair_recv, up_send, up_recv, down_send, down_recv, store = (
        sems.at[i] for i in range(8)
    )
    row = lax.axis_index("row")
    col = lax.axis_index("col")
    chip = col // 2
    core = col % 2
    other = col + 1 - 2 * core
    last = chips - 1
    half = max(chunks // 2, 1)
    lag = 2 if deal else 0
    depth = panel.shape[0]

    barrier = pltpu.get_barrier_semaphore()

    def greet(device):
        pl.semaphore_signal(barrier, inc=1, device_id=device, device_id_type=MESH)

    greet((row, other))

    @pl.when(chip > 0)
    def _():
        greet((row, col - 2))

    @pl.when(chip < last)
    def _():
        greet((row, col + 2))

    met = 1 + (chip > 0).astype(jnp.int32) + (chip < last).astype(jnp.int32)
    if deal:

        @pl.when(chip != row)
        def _():
            greet((chip, 2 * row))
            greet((chip, 2 * row + 1))

        met = met + 2 * (chip != row).astype(jnp.int32)
    pl.semaphore_wait(barrier, met)

    def span(j):
        if chunks == 1:
            return pl.ds(0, width)
        return pl.ds(pl.multiple_of(j * width, width), width)

    def load_copy(j):
        return pltpu.make_async_copy(part.at[:, core, :, span(j)], own.at[j], load.at[j])

    def remote(src, dst, send, recv, device):
        return pltpu.make_async_remote_copy(
            src_ref=src, dst_ref=dst, send_sem=send, recv_sem=recv,
            device_id=device, device_id_type=MESH,
        )

    def pair_copy(j):
        source = sent.at[j % 4] if deal else part.at[:, 1 - core, :, span(j)]
        return remote(source, pair.at[j], pair_send.at[j], pair_recv.at[j], (row, other))

    def fetch_copy(g):
        columns = pl.ds(pl.multiple_of(2 * g * width, 2 * width), 2 * width)
        return pltpu.make_async_copy(known.at[:, columns], fetched.at[g % 2], fetch.at[g % 2])

    def up_copy(j, at):
        units = pl.ds(at + 1, last - at)
        return remote(own.at[j, units], below.at[j, units], up_send.at[j], up_recv.at[j], (row, col + 2))

    def down_copy(j, at):
        units = pl.ds(0, at)
        return remote(own.at[j, units], above.at[j, units], down_send.at[j], down_recv.at[j], (row, col - 2))

    def store_copy(j):
        return pltpu.make_async_copy(own.at[j, chip], panel.at[:, span(j)], store.at[j])

    def kept(j):
        return (chip == row) & (j // half == core)

    def deal_spot(j):
        return dealt.at[core, j % half]

    def deal_copy(j):
        return remote(
            own.at[j, chip], deal_spot(j), deal_send.at[j], deal_recv.at[core, j % half],
            (chip, 2 * row + j // half),
        )

    def factor_copies(a):
        slot = a % 2
        at = pl.ds(pl.multiple_of(a * width, width), width)
        return [
            pltpu.make_async_copy(
                source.at[at, :], factors.at[slot, pl.ds(i * width, width)], factor_sems.at[slot, i]
            )
            for i, source in enumerate((sep, lead))
        ]

    def halves(x):
        rounded = x.astype(jnp.bfloat16)
        return rounded, (x - rounded.astype(jnp.float32)).astype(jnp.bfloat16)

    def begin(j, carry):
        load_copy(j).start()
        pair_copy(j).start()
        return carry

    if deal:
        fetch_copy(0).start()
        for copy in factor_copies(0):
            copy.start()
        total_copy = pltpu.make_async_copy(start, total, total_sem.at[0])
        total_copy.start()
        total_copy.wait()
    else:
        lax.fori_loop(0, chunks, begin, 0)

    def multiply(t):
        g = t // 2
        fetch_copy(g).wait()

        @pl.when(g + 1 < half)
        def _():
            fetch_copy(g + 1).start()

        @pl.when(t >= 4)
        def _():
            pair_copy(t - 4).wait_send()
            pair_copy(t - 3).wait_send()

        def split(i, carry):
            at = pl.ds(pl.multiple_of(i * 2 * width, 2 * width), 2 * width)
            block = fetched[g % 2, at, :]
            rounded = block.astype(jnp.bfloat16)
            known_high[at, :] = rounded
            known_low[at, :] = (block - rounded.astype(jnp.float32)).astype(jnp.bfloat16)
            return carry

        lax.fori_loop(0, fetched.shape[1] // (2 * width), split, 0)

        def unit(d, carry):
            at = pl.ds(pl.multiple_of(d * 2 * depth, 2 * depth), 2 * depth)
            total = jnp.dot(high[at, :], known_low[...], preferred_element_type=jnp.float32)
            total += jnp.dot(low[at, :], known_high[...], preferred_element_type=jnp.float32)
            total += jnp.dot(high[at, :], known_high[...], preferred_element_type=jnp.float32)
            for side in range(2):

                @pl.when(core == side)
                def _():
                    for i in range(2):
                        piece = total[:, i * width : (i + 1) * width]
                        own[t + i, d] = piece[side * depth : (side + 1) * depth]
                        sent[(t + i) % 4, d] = piece[(1 - side) * depth : (2 - side) * depth]

            return carry

        lax.fori_loop(0, chips, unit, 0)

    def accumulate(a):
        for i, copy in enumerate(factor_copies(a)):
            copy.wait()

        @pl.when(a + 1 < half)
        def _():
            for copy in factor_copies(a + 1):
                copy.start()

        for side in range(2):

            @pl.when(jnp.logical_not((chip == row) & (core == side)))
            def _():
                remote(
                    own.at[0, 0], dealt.at[side, a], deal_send.at[0], deal_recv.at[side, a],
                    (row, other),
                ).wait_recv()

        moved = jnp.concatenate([dealt[0, a], dealt[1, a]], axis=0)
        raised = moved * upper[...]
        moved_high, moved_low = halves(jnp.concatenate([moved - raised, -raised], axis=1))

        def column(n, carry):
            at = pl.ds(pl.multiple_of(n * 2 * width, 2 * width), 2 * width)
            factor_high, factor_low = halves(factors[a % 2, :, at])
            term = jnp.dot(moved_high, factor_low, preferred_element_type=jnp.float32)
            term += jnp.dot(moved_low, factor_high, preferred_element_type=jnp.float32)
            term += jnp.dot(moved_high, factor_high, preferred_element_type=jnp.float32)
            total[:, at] += term
            return carry

        lax.fori_loop(0, total.shape[1] // (2 * width), column, 0)

    def tick(t, carry):
        if deal:

            @pl.when((t < chunks) & (t % 2 == 0))
            def _():
                multiply(t)

        sum_at = t - lag

        @pl.when((sum_at >= 0) & (sum_at < chunks))
        def _():
            if not deal:
                load_copy(sum_at).wait()
            pair_copy(sum_at).wait_recv()
            own[sum_at] = own[sum_at] + pair[sum_at]

        if deal:

            @pl.when((t < chunks) & (t % 2 == 0))
            def _():
                pair_copy(t).start()
                pair_copy(t + 1).start()

        up = sum_at - chip
        down = sum_at - (last - chip)
        ready = sum_at - jnp.maximum(chip, last - chip)
        for at in range(chips):

            @pl.when((chip == at) & (up >= 0) & (up < chunks))
            def _():
                if at > 0:
                    up_copy(up, at - 1).wait_recv()
                    for d in range(at, chips):
                        own[up, d] = own[up, d] + below[up, d]

            @pl.when((chip == at) & (down >= 0) & (down < chunks))
            def _():
                if at < last:
                    down_copy(down, at + 1).wait_recv()
                    for d in range(at + 1):
                        own[down, d] = own[down, d] + above[down, d]

            @pl.when((chip == at) & (up >= 0) & (up < chunks))
            def _():
                if at < last:
                    up_copy(up, at).start()

            @pl.when((chip == at) & (down >= 0) & (down < chunks))
            def _():
                if at > 0:
                    down_copy(down, at).start()

        @pl.when((ready >= 0) & (ready < chunks))
        def _():
            store_copy(ready).start()
            if deal:

                @pl.when(kept(ready))
                def _():
                    dealt[core, ready % half] = own[ready, chip]

                @pl.when(jnp.logical_not(kept(ready)))
                def _():
                    deal_copy(ready).start()

        if deal:
            arrival = sum_at - jnp.maximum(row, last - row) - 2 - core * half

            @pl.when((arrival >= 0) & (arrival < half))
            def _():
                accumulate(arrival)

        return carry

    lax.fori_loop(0, chunks + last + 2 * lag, tick, 0)

    def finish(j, carry):
        @pl.when(j >= (chunks - 4 if deal else 0))
        def _():
            pair_copy(j).wait_send()

        store_copy(j).wait()
        for at in range(chips):

            @pl.when(chip == at)
            def _():
                if at < last:
                    up_copy(j, at).wait_send()
                if at > 0:
                    down_copy(j, at).wait_send()

        if deal:

            @pl.when(jnp.logical_not(kept(j)))
            def _():
                deal_copy(j).wait_send()

        return carry

    lax.fori_loop(0, chunks, finish, 0)
    if deal:
        total_copy = pltpu.make_async_copy(total, product, total_sem.at[0])
        total_copy.start()
        total_copy.wait()


ANYWHERE = pl.BlockSpec(memory_space=pl.ANY)
IN_VMEM = pl.BlockSpec(memory_space=pltpu.VMEM)


def line_params(number):
    return pltpu.CompilerParams(
        collective_id=number, has_side_effects=True, vmem_limit_bytes=62 << 20
    )


def line_scratch(chunks, chips, depth, width):
    block = pltpu.VMEM((chunks, chips, depth, width), jnp.float32)
    return [block] * 4 + [pltpu.SemaphoreType.DMA((8, chunks))]


def panel_reduce(high, low, known, sep, lead, start, upper, chips):
    inner, wide = known.shape
    depth = start.shape[0] // 2
    width = 128
    chunks = wide // width
    return pl.pallas_call(
        functools.partial(line_kernel, chunks, chips, width, True),
        out_shape=[
            jax.ShapeDtypeStruct((depth, wide), jnp.float32),
            jax.ShapeDtypeStruct(start.shape, jnp.float32),
        ],
        in_specs=[IN_VMEM] * 2 + [ANYWHERE] * 4 + [IN_VMEM],
        out_specs=[ANYWHERE] * 2,
        scratch_shapes=line_scratch(chunks, chips, depth, width)
        + [
            pltpu.SemaphoreType.DMA((chunks,)),
            pltpu.SemaphoreType.DMA((2, chunks // 2)),
            pltpu.VMEM((2, inner, 2 * width), jnp.float32),
            pltpu.VMEM((inner, 2 * width), jnp.bfloat16),
            pltpu.VMEM((inner, 2 * width), jnp.bfloat16),
            pltpu.VMEM((4, chips, depth, width), jnp.float32),
            pltpu.SemaphoreType.DMA((2,)),
            pltpu.VMEM((2, chunks // 2, depth, width), jnp.float32),
            pltpu.VMEM((2, 2 * width, start.shape[1]), jnp.float32),
            pltpu.VMEM(start.shape, jnp.float32),
            pltpu.SemaphoreType.DMA((2, 2)),
            pltpu.SemaphoreType.DMA((1,)),
        ],
        compiler_params=line_params(1),
        name="panel_reduce",
    )(high, low, known, sep, lead, start, jnp.broadcast_to(upper[:, None], (2 * depth, width)))


def block_reduce(part):
    chips, _, depth, wide = part.shape
    chunks = wide // 128 if wide % 128 == 0 else 1
    return pl.pallas_call(
        functools.partial(line_kernel, chunks, chips, wide // chunks, False),
        out_shape=jax.ShapeDtypeStruct((depth, wide), jnp.float32),
        in_specs=[ANYWHERE],
        out_specs=ANYWHERE,
        scratch_shapes=line_scratch(chunks, chips, depth, wide // chunks),
        compiler_params=line_params(2),
        name="block_reduce",
    )(part)


def plane_kernel(rows, part, total, arrived, sends, recvs):
    row = lax.axis_index("row")
    col = lax.axis_index("col")
    tall = total.shape[1]
    barrier = pltpu.get_barrier_semaphore()
    for step in range(1, rows):
        device = (lax.rem(row + step, rows), col)
        pl.semaphore_signal(barrier, inc=1, device_id=device, device_id_type=MESH)
    pl.semaphore_wait(barrier, rows - 1)

    def copy(step):
        target = lax.rem(row + step, rows)
        columns = pl.ds(pl.multiple_of(target * tall, tall), tall)
        return pltpu.make_async_remote_copy(
            src_ref=part.at[:, columns], dst_ref=arrived.at[step],
            send_sem=sends.at[step], recv_sem=recvs.at[step],
            device_id=(target, col), device_id_type=MESH,
        )

    for step in range(1, rows):
        copy(step).start()
    columns = pl.ds(pl.multiple_of(row * tall, tall), tall)
    mine = pltpu.make_async_copy(part.at[:, columns], arrived.at[0], recvs.at[0])
    mine.start()
    mine.wait()
    for step in range(1, rows):
        copy(step).wait()
    result = arrived[0]
    for step in range(1, rows):
        result = result + arrived[step]
    total[...] = result


def plane_reduce(part, rows):
    depth, wide = part.shape
    tall = wide // rows
    if tall % 128:
        return lax.psum_scatter(part, "row", scatter_dimension=1, tiled=True)
    return pl.pallas_call(
        functools.partial(plane_kernel, rows),
        out_shape=jax.ShapeDtypeStruct((depth, tall), jnp.float32),
        in_specs=[ANYWHERE],
        out_specs=pl.BlockSpec(memory_space=pltpu.VMEM),
        scratch_shapes=[
            pltpu.VMEM((rows, depth, tall), jnp.float32),
            pltpu.SemaphoreType.DMA((rows,)),
            pltpu.SemaphoreType.DMA((rows,)),
        ],
        compiler_params=line_params(3),
        name="plane_reduce",
    )(part)


def gather_kernel(chips, mine, out, held, sems, stores):
    row = lax.axis_index("row")
    col = lax.axis_index("col")
    chip = col // 2
    core = col % 2
    other = col + 1 - 2 * core
    last = chips - 1
    piece = held.shape[2] // 2
    along_x, along_y, across = row + 1 - 2 * (row % 2), (row + 2) % 4, 3 - row

    barrier = pltpu.get_barrier_semaphore()

    def greet(device):
        pl.semaphore_signal(barrier, inc=1, device_id=device, device_id_type=MESH)

    greet((row, other))
    greet((along_x, col))
    greet((along_y, col))

    @pl.when(chip > 0)
    def _():
        greet((row, col - 2))

    @pl.when(chip < last)
    def _():
        greet((row, col + 2))

    met = 3 + (chip > 0).astype(jnp.int32) + (chip < last).astype(jnp.int32)
    pl.semaphore_wait(barrier, met)

    def remote(at, quarter, side, send, recv, device):
        ref = held.at[2 * at + core, quarter, pl.ds(side * piece, piece)]
        spot = 2 * at + side
        return pltpu.make_async_remote_copy(
            src_ref=ref, dst_ref=ref, send_sem=sems.at[send, spot], recv_sem=sems.at[recv, spot],
            device_id=device, device_id_type=MESH,
        )

    def up(at, side):
        return remote(at, row, side, 0, 2, (row, col + 2))

    def down(at, side):
        return remote(at, row, side, 1, 2, (row, col - 2))

    def sideways_x(at, side):
        return remote(at, row, side, 3, 4, (along_x, col))

    def sideways_y(at, side):
        return remote(at, row, side, 5, 6, (along_y, col))

    def onward_x(at):
        return remote(at, along_y, 0, 7, 8, (along_x, col))

    def onward_y(at):
        return remote(at, along_x, 1, 7, 8, (along_y, col))

    def hand(at, quarter, side):
        return remote(at, quarter, side, 9 + quarter, 13 + quarter, (row, other))

    def hand_own():
        return pltpu.make_async_remote_copy(
            src_ref=held.at[col], dst_ref=held.at[col], send_sem=sems.at[17, 0],
            recv_sem=sems.at[18, 0], device_id=(row, other), device_id_type=MESH,
        )

    def keep(c):
        return pltpu.make_async_copy(held.at[c], out.at[c], stores.at[c])

    def both_ways(visit):
        for distance in range(1, chips):

            @pl.when(chip - distance >= 0)
            def _():
                visit(chip - distance, True)

            @pl.when(chip + distance <= last)
            def _():
                visit(chip + distance, False)

    load = pltpu.make_async_copy(mine, held.at[col], sems.at[19, 0])
    load.start()
    load.wait()

    def send_line(at, side, rising):
        if rising:

            @pl.when(chip < last)
            def _():
                up(at, side).start()

        else:

            @pl.when(chip > 0)
            def _():
                down(at, side).start()

    for side in range(2):
        send_line(chip, side, True)
        send_line(chip, side, False)
    hand_own().start()
    keep(col).start()

    def from_line(at, rising):
        for side in range(2):
            up(at, side).wait_recv()
            send_line(at, side, rising)
            sideways_x(at, side).start()
            sideways_y(at, side).start()
            hand(at, row, side).start()

    def from_sides(at, rising):
        for side in range(2):
            sideways_x(at, side).wait_recv()
            if side == 1:
                onward_y(at).start()
            sideways_y(at, side).wait_recv()
            if side == 0:
                onward_x(at).start()
            hand(at, along_x, side).start()
            hand(at, along_y, side).start()

    def from_across(at, rising):
        onward_x(at).wait_recv()
        hand(at, across, 0).start()
        onward_y(at).wait_recv()
        hand(at, across, 1).start()
        keep(2 * at + core).start()

    def from_other(at, rising):
        for quarter in range(4):
            for side in range(2):
                hand(at, quarter, side).wait_recv()
        keep(2 * at + 1 - core).start()

    both_ways(from_line)
    both_ways(from_sides)
    both_ways(from_across)
    hand_own().wait_recv()
    keep(other).start()
    both_ways(from_other)

    def drain_line(at, side, rising):
        if rising:

            @pl.when(chip < last)
            def _():
                up(at, side).wait_send()

        else:

            @pl.when(chip > 0)
            def _():
                down(at, side).wait_send()

    def drain(at, rising):
        for side in range(2):
            drain_line(at, side, rising)
            sideways_x(at, side).wait_send()
            sideways_y(at, side).wait_send()
            for quarter in range(4):
                hand(at, quarter, side).wait_send()
        onward_x(at).wait_send()
        onward_y(at).wait_send()

    both_ways(drain)
    for side in range(2):
        drain_line(chip, side, True)
        drain_line(chip, side, False)
    hand_own().wait_send()
    for c in range(2 * chips):
        keep(c).wait()


def gather_rows(mine, rows, cols):
    depth, wide = mine.shape
    piece = depth // 4
    if rows != 4 or piece % 16:
        return lax.all_gather(mine, "col", axis=0, tiled=True)
    shape = (cols, 4, piece, wide)
    out = pl.pallas_call(
        functools.partial(gather_kernel, cols // 2),
        out_shape=jax.ShapeDtypeStruct(shape, jnp.float32),
        in_specs=[ANYWHERE],
        out_specs=ANYWHERE,
        scratch_shapes=[
            pltpu.VMEM(shape, jnp.float32),
            pltpu.SemaphoreType.DMA((20, cols)),
            pltpu.SemaphoreType.DMA((cols,)),
        ],
        compiler_params=line_params(4),
        name="gather_rows",
    )(mine.reshape(4, piece, wide))
    return out.reshape(cols * depth, wide)


def lead_kernel(tile, flags, factor, listed, upper, coupling, high, low, lead, sep, *scratch):
    upper_high, upper_low, total = scratch
    wide = factor.shape[1]
    block = factor.shape[0] // listed.shape[1]

    for i in range(listed.shape[1]):
        at = pl.ds(i * block, block)
        sep[at, :] = factor[at, :] * listed[0, i : i + 1, :]

    def split(x):
        rounded = x.astype(jnp.bfloat16)
        return rounded, (x - rounded.astype(jnp.float32)).astype(jnp.bfloat16)

    def prepare(k, carry):
        at = pl.ds(pl.multiple_of(k * tile, tile), tile)
        upper_high[:, at], upper_low[:, at] = split(sep[:, at] * upper[:, at])
        return carry

    lax.fori_loop(0, wide // tile, prepare, 0)

    def column(m, carry):
        at = pl.ds(pl.multiple_of(m * tile, tile), tile)
        total[...] = -sep[:, at]

        def inner(k, carry):
            @pl.when(flags[k, m] != 0)
            def _():
                along = pl.ds(pl.multiple_of(k * tile, tile), tile)
                pair_high, pair_low = split(coupling[along, at])

                def times(left, right):
                    return jnp.dot(left[:, along], right, preferred_element_type=jnp.float32)

                term = times(upper_high, pair_low) + times(upper_low, pair_high)
                total[...] += term + times(upper_high, pair_high)

            return carry

        lax.fori_loop(0, wide // tile, inner, 0)
        lead[:, at] = total[...]
        high[at, :], low[at, :] = split(total[...].T)
        return carry

    lax.fori_loop(0, wide // tile, column, 0)


def lead_factors(factor, listed, upper, coupling, flags):
    tall, wide = factor.shape
    block = tall // listed.shape[0]
    step = 2 * block
    tile = wide // flags.shape[0]
    turned = pl.BlockSpec((wide, step), lambda i, f: (0, i))
    straight = pl.BlockSpec((step, wide), lambda i, f: (i, 0))
    return pl.pallas_call(
        functools.partial(lead_kernel, tile),
        out_shape=[jax.ShapeDtypeStruct((wide, tall), jnp.bfloat16)] * 2
        + [jax.ShapeDtypeStruct((tall, wide), jnp.float32)] * 2,
        grid_spec=pltpu.PrefetchScalarGridSpec(
            num_scalar_prefetch=1,
            grid=(tall // step,),
            in_specs=[
                straight,
                pl.BlockSpec((1, 2, wide), lambda i, f: (i, 0, 0)),
                pl.BlockSpec((1, wide), lambda i, f: (0, 0)),
                pl.BlockSpec((wide, wide), lambda i, f: (0, 0), pipeline_mode=pl.Buffered(1)),
            ],
            out_specs=[turned, turned, straight, straight],
            scratch_shapes=[
                pltpu.VMEM((step, wide), jnp.bfloat16),
                pltpu.VMEM((step, wide), jnp.bfloat16),
                pltpu.VMEM((step, tile), jnp.float32),
            ],
        ),
        compiler_params=pltpu.CompilerParams(vmem_limit_bytes=62 << 20),
        name="lead_factors",
    )(flags, factor, listed.reshape(-1, 2, wide), upper[None, :], coupling)


def shards(known_inverse, factor_sep, factor_pair, pivot_inverse, widths, parent_of, ancestors):
    col_index = lax.axis_index("col")
    row_index = lax.axis_index("row")
    rows = lax.axis_size("row")
    cols = lax.axis_size("col")
    chips = cols // 2
    chip, core = col_index // 2, col_index % 2
    sep_local = factor_sep.shape[0]
    pair_local = factor_pair.shape[0]
    wide_local = pivot_inverse.shape[1]
    column_owner, column_blocks, column_parent, column_upper = supernode_tables(
        widths, parent_of, ancestors
    )

    def rows_of(x, index, size):
        return lax.dynamic_slice_in_dim(x, index * size, size)

    def cols_of(x, index, size):
        return lax.dynamic_slice_in_dim(x, index * size, size, 1)

    blocks = sep_local // (NS // NBLK)
    listed = lax.dynamic_slice_in_dim(column_blocks, col_index * blocks, blocks, 1).T
    upper_cols = column_upper.astype(jnp.float32)
    owner_rows = rows_of(column_owner, col_index, pair_local)
    owner_wide = rows_of(column_owner, row_index, wide_local)
    parent_wide = rows_of(column_parent, row_index, wide_local)
    upper_wide = rows_of(column_upper, row_index, wide_local)
    coupling = jnp.where(
        (owner_rows[:, None] == column_parent[None, :]) & (~column_upper)[None, :], factor_pair, 0.0
    )
    matching = owner_rows[:, None] == owner_wide[None, :]
    match_pair = owner_rows[:, None] == parent_wide[None, :]

    coupling_all = gather_rows(coupling, rows, cols)

    straight = [
        (r * cols + 2 * z + q, z * cols + 2 * r + q)
        for r in range(rows)
        for z in range(chips)
        for q in range(2)
    ]
    crossed = [(source, target ^ 1) for source, target in straight]
    swapped = [(device, device ^ 1) for device in range(rows * cols)]

    def permute(x, order):
        return lax.ppermute(x, ("row", "col"), order)

    def ordered(mine, others):
        return jnp.where(
            core == 0, jnp.concatenate([mine, others]), jnp.concatenate([others, mine])
        )

    upper_pivot = jnp.where(matching & upper_wide[None, :], pivot_inverse, 0.0)
    pivot_tile = ordered(
        permute(cols_of(upper_pivot, core, pair_local), straight),
        permute(cols_of(upper_pivot, 1 - core, pair_local), crossed),
    )
    pivot_coupled = plain_dot(pivot_tile, coupling)

    nodes = jnp.arange(NSUP, dtype=jnp.int32)
    tiles = WTOT // 256
    holds = jnp.any(column_owner.reshape(tiles, 256, 1) == nodes, axis=1)
    wants = jnp.any(column_parent.reshape(tiles, 256, 1) == nodes, axis=1)
    flags = jnp.any(holds[:, None, :] & wants[None, :, :], axis=2).astype(jnp.int32)
    high, low, lead, sep_factor = lead_factors(
        factor_sep, listed, upper_cols, coupling_all, flags
    )
    panel, product = panel_reduce(
        high,
        low,
        known_inverse,
        sep_factor,
        lead,
        pivot_coupled,
        upper_wide.astype(jnp.float32),
        chips,
    )
    product = product.reshape(2, pair_local, chips, wide_local).transpose(2, 0, 1, 3)
    tile = block_reduce(product)

    dealt_tile = permute(tile, straight)
    pair_tile = jnp.where(
        rows_of(column_owner, 2 * row_index + core, pair_local)[:, None]
        == rows_of(column_parent, chip, wide_local)[None, :],
        -tile,
        0.0,
    )
    pair_cols = ordered(
        cols_of(pair_tile, core, pair_local),
        permute(cols_of(pair_tile, 1 - core, pair_local), swapped),
    )
    below = first_dot(pair_cols, rows_of(coupling_all, row_index, wide_local))
    below = plane_reduce(below, rows)

    own_block = jnp.where(
        matching, pivot_inverse - dealt_tile - jnp.where(upper_wide[None, :], 0.0, below), 0.0
    )
    return panel, own_block + jnp.where(match_pair, -dealt_tile, 0.0)


def solution(mesh):
    if mesh.shape["col"] != 2 * mesh.shape["row"]:
        raise ValueError("unsupported mesh")
    in_specs = (P("col", "row"), P("col", None), P("col", None), P("col", "row"), P(), P(), P())
    out_specs = (P("col", "row"), P("col", "row"))
    return jax.shard_map(shards, mesh=mesh, in_specs=in_specs, out_specs=out_specs, check_vma=False)
```

```python
import functools

import jax
import jax.numpy as jnp
from jax import lax
from jax.experimental import pallas as pl
from jax.experimental.pallas import tpu as pltpu
from jax.sharding import PartitionSpec as P

NS = 12288
WTOT = 1536
NSUP = 8
NBLK = 64

MESH = pl.DeviceIdType.MESH
exact_mode = lax.Precision.HIGH


def plain_dot(left, right):
    return jnp.dot(left, right, precision=exact_mode, preferred_element_type=jnp.float32)


def first_dot(left, right):
    return lax.dot_general(
        left,
        right,
        (((0,), (0,)), ((), ())),
        precision=exact_mode,
        preferred_element_type=jnp.float32,
    )

def supernode_tables(widths, parent_of, ancestors):
    position = jnp.arange(WTOT, dtype=jnp.int32)
    earlier = jnp.arange(NSUP)[None, :] <= jnp.arange(NSUP)[:, None]
    width_ends = jnp.sum(jnp.where(earlier, widths[None, :], 0), axis=1)
    column_owner = jnp.sum((width_ends[None, :] <= position[:, None]).astype(jnp.int32), axis=1)
    owner_onehot = column_owner[:, None] == jnp.arange(NSUP, dtype=jnp.int32)[None, :]
    listed = jnp.any(
        ancestors[:, :, None] == jnp.arange(NBLK, dtype=jnp.int32)[None, None, :], axis=1
    ).astype(jnp.float32)
    column_blocks = plain_dot(owner_onehot.astype(jnp.float32), listed)
    column_parent = jnp.sum(jnp.where(owner_onehot, parent_of[None, :], 0), axis=1)
    column_upper = column_parent < 0
    return (column_owner, column_blocks, column_parent, column_upper)


def line_kernel(chunks, chips, width, deal, *refs):
    if deal:
        high, low, known, sep, lead, start, upper, panel, product, *refs = refs
        own, pair, below, above, sems, *refs = refs
        deal_send, deal_recv, fetched, known_high, known_low, sent, fetch, *refs = refs
        dealt, factors, total, factor_sems, total_sem = refs
    else:
        part, panel, own, pair, below, above, sems, unit_sems = refs
        flat = len(part.shape) == 3
    load, pair_send, pair_recv, up_send, up_recv, down_send, down_recv, store = (
        sems.at[i] for i in range(8)
    )
    row = lax.axis_index("row")
    col = lax.axis_index("col")
    chip = col // 2
    core = col % 2
    other = col + 1 - 2 * core
    last = chips - 1
    half = max(chunks // 2, 1)
    lag = 2 if deal else 0
    depth = panel.shape[0]

    barrier = pltpu.get_barrier_semaphore()

    def greet(device):
        pl.semaphore_signal(barrier, inc=1, device_id=device, device_id_type=MESH)

    greet((row, other))

    @pl.when(chip > 0)
    def _():
        greet((row, col - 2))

    @pl.when(chip < last)
    def _():
        greet((row, col + 2))

    met = 1 + (chip > 0).astype(jnp.int32) + (chip < last).astype(jnp.int32)
    if deal:

        @pl.when(chip != row)
        def _():
            greet((chip, 2 * row))
            greet((chip, 2 * row + 1))

        met = met + 2 * (chip != row).astype(jnp.int32)
    def span(j):
        if chunks == 1:
            return pl.ds(0, width)
        return pl.ds(pl.multiple_of(j * width, width), width)

    def unit_span(j, d):
        at = d * panel.shape[1] + j * width
        return pl.ds(pl.multiple_of(at, width), width)

    def load_copies(j):
        if flat:
            return [
                pltpu.make_async_copy(
                    part.at[core, :, unit_span(j, d)], own.at[j, d], unit_sems.at[0, j, d]
                )
                for d in range(chips)
            ]
        return [pltpu.make_async_copy(part.at[:, core, :, span(j)], own.at[j], load.at[j])]

    def remote(src, dst, send, recv, device):
        return pltpu.make_async_remote_copy(
            src_ref=src, dst_ref=dst, send_sem=send, recv_sem=recv,
            device_id=device, device_id_type=MESH,
        )

    def pair_copies(j):
        if not deal and flat:
            return [
                remote(
                    part.at[1 - core, :, unit_span(j, d)], pair.at[j, d],
                    unit_sems.at[1, j, d], unit_sems.at[2, j, d], (row, other),
                )
                for d in range(chips)
            ]
        source = sent.at[j % 4] if deal else part.at[:, 1 - core, :, span(j)]
        return [remote(source, pair.at[j], pair_send.at[j], pair_recv.at[j], (row, other))]

    def fetch_copy(g):
        columns = pl.ds(pl.multiple_of(2 * g * width, 2 * width), 2 * width)
        return pltpu.make_async_copy(known.at[:, columns], fetched.at[g % 2], fetch.at[g % 2])

    def up_copy(j, at):
        units = pl.ds(at + 1, last - at)
        return remote(own.at[j, units], below.at[j, units], up_send.at[j], up_recv.at[j], (row, col + 2))

    def down_copy(j, at):
        units = pl.ds(0, at)
        return remote(own.at[j, units], above.at[j, units], down_send.at[j], down_recv.at[j], (row, col - 2))

    def store_copy(j):
        return pltpu.make_async_copy(own.at[j, chip], panel.at[:, span(j)], store.at[j])

    def kept(j):
        return (chip == row) & (j // half == core)

    def deal_spot(j):
        return dealt.at[core, j % half]

    def deal_copy(j):
        return remote(
            own.at[j, chip], deal_spot(j), deal_send.at[j], deal_recv.at[core, j % half],
            (chip, 2 * row + j // half),
        )

    def factor_copies(a):
        slot = a % 2
        at = pl.ds(pl.multiple_of(a * width, width), width)
        return [
            pltpu.make_async_copy(
                source.at[at, :], factors.at[slot, pl.ds(i * width, width)], factor_sems.at[slot, i]
            )
            for i, source in enumerate((sep, lead))
        ]

    def halves(x):
        rounded = x.astype(jnp.bfloat16)
        return rounded, (x - rounded.astype(jnp.float32)).astype(jnp.bfloat16)

    if deal:
        fetch_copy(0).start()
        for copy in factor_copies(0):
            copy.start()
        total_copy = pltpu.make_async_copy(start, total, total_sem.at[0])
        total_copy.start()
        pl.semaphore_wait(barrier, met)
    else:
        for j in range(chunks):
            for copy in load_copies(j):
                copy.start()
        pl.semaphore_wait(barrier, met)
        for j in range(chunks):
            for copy in pair_copies(j):
                copy.start()

    def multiply(t):
        g = t // 2
        fetch_copy(g).wait()

        @pl.when(g + 1 < half)
        def _():
            fetch_copy(g + 1).start()

        @pl.when(t >= 4)
        def _():
            for copy in pair_copies(t - 4) + pair_copies(t - 3):
                copy.wait_send()

        def split(i, carry):
            at = pl.ds(pl.multiple_of(i * 2 * width, 2 * width), 2 * width)
            block = fetched[g % 2, at, :]
            rounded = block.astype(jnp.bfloat16)
            known_high[at, :] = rounded
            known_low[at, :] = (block - rounded.astype(jnp.float32)).astype(jnp.bfloat16)
            return carry

        lax.fori_loop(0, fetched.shape[1] // (2 * width), split, 0)

        def unit(d, carry):
            at = pl.ds(pl.multiple_of(d * 2 * depth, 2 * depth), 2 * depth)
            total = jnp.dot(high[at, :], known_low[...], preferred_element_type=jnp.float32)
            total += jnp.dot(low[at, :], known_high[...], preferred_element_type=jnp.float32)
            total += jnp.dot(high[at, :], known_high[...], preferred_element_type=jnp.float32)
            for side in range(2):

                @pl.when(core == side)
                def _():
                    for i in range(2):
                        piece = total[:, i * width : (i + 1) * width]
                        own[t + i, d] = piece[side * depth : (side + 1) * depth]
                        sent[(t + i) % 4, d] = piece[(1 - side) * depth : (2 - side) * depth]

            return carry

        lax.fori_loop(0, chips, unit, 0)

    def accumulate(a):
        @pl.when(a == 0)
        def _():
            total_copy.wait()

        for i, copy in enumerate(factor_copies(a)):
            copy.wait()

        @pl.when(a + 1 < half)
        def _():
            for copy in factor_copies(a + 1):
                copy.start()

        for side in range(2):

            @pl.when(jnp.logical_not((chip == row) & (core == side)))
            def _():
                remote(
                    own.at[0, 0], dealt.at[side, a], deal_send.at[0], deal_recv.at[side, a],
                    (row, other),
                ).wait_recv()

        moved = jnp.concatenate([dealt[0, a], dealt[1, a]], axis=0)
        raised = moved * upper[...]
        moved_high, moved_low = halves(jnp.concatenate([moved - raised, -raised], axis=1))

        def column(n, carry):
            at = pl.ds(pl.multiple_of(n * 2 * width, 2 * width), 2 * width)
            factor_high, factor_low = halves(factors[a % 2, :, at])
            term = jnp.dot(moved_high, factor_low, preferred_element_type=jnp.float32)
            term += jnp.dot(moved_low, factor_high, preferred_element_type=jnp.float32)
            term += jnp.dot(moved_high, factor_high, preferred_element_type=jnp.float32)
            total[:, at] += term
            return carry

        lax.fori_loop(0, total.shape[1] // (2 * width), column, 0)

    def tick(t, carry):
        if deal:

            @pl.when((t < chunks) & (t % 2 == 0))
            def _():
                multiply(t)

        sum_at = t - lag

        @pl.when((sum_at >= 0) & (sum_at < chunks))
        def _():
            if not deal:
                for copy in load_copies(sum_at):
                    copy.wait()
            for copy in pair_copies(sum_at):
                copy.wait_recv()
            own[sum_at] = own[sum_at] + pair[sum_at]

        if deal:

            @pl.when((t < chunks) & (t % 2 == 0))
            def _():
                for copy in pair_copies(t) + pair_copies(t + 1):
                    copy.start()

        up = sum_at - chip
        down = sum_at - (last - chip)
        ready = sum_at - jnp.maximum(chip, last - chip)
        for at in range(chips):

            @pl.when((chip == at) & (up >= 0) & (up < chunks))
            def _():
                if at > 0:
                    up_copy(up, at - 1).wait_recv()
                    for d in range(at, chips):
                        own[up, d] = own[up, d] + below[up, d]

            @pl.when((chip == at) & (down >= 0) & (down < chunks))
            def _():
                if at < last:
                    down_copy(down, at + 1).wait_recv()
                    for d in range(at + 1):
                        own[down, d] = own[down, d] + above[down, d]

            @pl.when((chip == at) & (up >= 0) & (up < chunks))
            def _():
                if at < last:
                    up_copy(up, at).start()

            @pl.when((chip == at) & (down >= 0) & (down < chunks))
            def _():
                if at > 0:
                    down_copy(down, at).start()

        @pl.when((ready >= 0) & (ready < chunks))
        def _():
            store_copy(ready).start()
            if deal:

                @pl.when(kept(ready))
                def _():
                    dealt[core, ready % half] = own[ready, chip]

                @pl.when(jnp.logical_not(kept(ready)))
                def _():
                    deal_copy(ready).start()

        if deal:
            arrival = sum_at - jnp.maximum(row, last - row) - 2 - core * half

            @pl.when((arrival >= 0) & (arrival < half))
            def _():
                accumulate(arrival)

        return carry

    lax.fori_loop(0, chunks + last + 2 * lag, tick, 0)

    def finish(j, carry):
        @pl.when(j >= (chunks - 4 if deal else 0))
        def _():
            for copy in pair_copies(j):
                copy.wait_send()

        store_copy(j).wait()
        for at in range(chips):

            @pl.when(chip == at)
            def _():
                if at < last:
                    up_copy(j, at).wait_send()
                if at > 0:
                    down_copy(j, at).wait_send()

        if deal:

            @pl.when(jnp.logical_not(kept(j)))
            def _():
                deal_copy(j).wait_send()

        return carry

    lax.fori_loop(0, chunks, finish, 0)
    if deal:
        total_copy = pltpu.make_async_copy(total, product, total_sem.at[0])
        total_copy.start()
        total_copy.wait()


ANYWHERE = pl.BlockSpec(memory_space=pl.ANY)
IN_VMEM = pl.BlockSpec(memory_space=pltpu.VMEM)


def line_params(number):
    return pltpu.CompilerParams(
        collective_id=number, has_side_effects=True, vmem_limit_bytes=62 << 20
    )


def line_scratch(chunks, chips, depth, width):
    block = pltpu.VMEM((chunks, chips, depth, width), jnp.float32)
    return [block] * 4 + [pltpu.SemaphoreType.DMA((8, chunks))]


def panel_reduce(high, low, known, sep, lead, start, upper, chips):
    inner, wide = known.shape
    depth = start.shape[0] // 2
    width = 128
    chunks = wide // width
    return pl.pallas_call(
        functools.partial(line_kernel, chunks, chips, width, True),
        out_shape=[
            jax.ShapeDtypeStruct((depth, wide), jnp.float32),
            jax.ShapeDtypeStruct(start.shape, jnp.float32),
        ],
        in_specs=[IN_VMEM] * 2 + [ANYWHERE] * 4 + [IN_VMEM],
        out_specs=[ANYWHERE] * 2,
        scratch_shapes=line_scratch(chunks, chips, depth, width)
        + [
            pltpu.SemaphoreType.DMA((chunks,)),
            pltpu.SemaphoreType.DMA((2, chunks // 2)),
            pltpu.VMEM((2, inner, 2 * width), jnp.float32),
            pltpu.VMEM((inner, 2 * width), jnp.bfloat16),
            pltpu.VMEM((inner, 2 * width), jnp.bfloat16),
            pltpu.VMEM((4, chips, depth, width), jnp.float32),
            pltpu.SemaphoreType.DMA((2,)),
            pltpu.VMEM((2, chunks // 2, depth, width), jnp.float32),
            pltpu.VMEM((2, 2 * width, start.shape[1]), jnp.float32),
            pltpu.VMEM(start.shape, jnp.float32),
            pltpu.SemaphoreType.DMA((2, 2)),
            pltpu.SemaphoreType.DMA((1,)),
        ],
        compiler_params=line_params(1),
        name="panel_reduce",
    )(high, low, known, sep, lead, start, jnp.broadcast_to(upper[:, None], (2 * depth, width)))


def block_reduce(product, chips):
    tall, wide = product.shape
    depth, wide = tall // 2, wide // chips
    if wide % 128:
        part = product.reshape(2, depth, chips, wide).transpose(2, 0, 1, 3)
        width = wide
    else:
        part = product.reshape(2, depth, chips * wide)
        width = 128
    chunks = wide // width
    return pl.pallas_call(
        functools.partial(line_kernel, chunks, chips, width, False),
        out_shape=jax.ShapeDtypeStruct((depth, wide), jnp.float32),
        in_specs=[ANYWHERE],
        out_specs=ANYWHERE,
        scratch_shapes=line_scratch(chunks, chips, depth, width)
        + [pltpu.SemaphoreType.DMA((3, chunks, chips))],
        compiler_params=line_params(2),
        name="block_reduce",
    )(part)


def plane_kernel(rows, part, total, arrived, sends, recvs):
    row = lax.axis_index("row")
    col = lax.axis_index("col")
    tall = total.shape[1]
    barrier = pltpu.get_barrier_semaphore()
    for step in range(1, rows):
        device = (lax.rem(row + step, rows), col)
        pl.semaphore_signal(barrier, inc=1, device_id=device, device_id_type=MESH)
    pl.semaphore_wait(barrier, rows - 1)

    def copy(step):
        target = lax.rem(row + step, rows)
        columns = pl.ds(pl.multiple_of(target * tall, tall), tall)
        return pltpu.make_async_remote_copy(
            src_ref=part.at[:, columns], dst_ref=arrived.at[step],
            send_sem=sends.at[step], recv_sem=recvs.at[step],
            device_id=(target, col), device_id_type=MESH,
        )

    for step in range(1, rows):
        copy(step).start()
    columns = pl.ds(pl.multiple_of(row * tall, tall), tall)
    mine = pltpu.make_async_copy(part.at[:, columns], arrived.at[0], recvs.at[0])
    mine.start()
    mine.wait()
    for step in range(1, rows):
        copy(step).wait()
    result = arrived[0]
    for step in range(1, rows):
        result = result + arrived[step]
    total[...] = result


def plane_reduce(part, rows):
    depth, wide = part.shape
    tall = wide // rows
    if tall % 128:
        return lax.psum_scatter(part, "row", scatter_dimension=1, tiled=True)
    return pl.pallas_call(
        functools.partial(plane_kernel, rows),
        out_shape=jax.ShapeDtypeStruct((depth, tall), jnp.float32),
        in_specs=[ANYWHERE],
        out_specs=pl.BlockSpec(memory_space=pltpu.VMEM),
        scratch_shapes=[
            pltpu.VMEM((rows, depth, tall), jnp.float32),
            pltpu.SemaphoreType.DMA((rows,)),
            pltpu.SemaphoreType.DMA((rows,)),
        ],
        compiler_params=line_params(3),
        name="plane_reduce",
    )(part)


def gather_kernel(chips, mine, out, held, sems, stores):
    row = lax.axis_index("row")
    col = lax.axis_index("col")
    chip = col // 2
    core = col % 2
    other = col + 1 - 2 * core
    last = chips - 1
    piece = held.shape[2] // 2
    along_x, along_y, across = row + 1 - 2 * (row % 2), (row + 2) % 4, 3 - row

    barrier = pltpu.get_barrier_semaphore()

    def greet(device):
        pl.semaphore_signal(barrier, inc=1, device_id=device, device_id_type=MESH)

    greet((row, other))
    greet((along_x, col))
    greet((along_y, col))

    @pl.when(chip > 0)
    def _():
        greet((row, col - 2))

    @pl.when(chip < last)
    def _():
        greet((row, col + 2))

    met = 3 + (chip > 0).astype(jnp.int32) + (chip < last).astype(jnp.int32)
    pl.semaphore_wait(barrier, met)

    def remote(at, quarter, side, send, recv, device):
        ref = held.at[2 * at + core, quarter, pl.ds(side * piece, piece)]
        spot = 2 * at + side
        return pltpu.make_async_remote_copy(
            src_ref=ref, dst_ref=ref, send_sem=sems.at[send, spot], recv_sem=sems.at[recv, spot],
            device_id=device, device_id_type=MESH,
        )

    def up(at, side):
        return remote(at, row, side, 0, 2, (row, col + 2))

    def down(at, side):
        return remote(at, row, side, 1, 2, (row, col - 2))

    def sideways_x(at, side):
        return remote(at, row, side, 3, 4, (along_x, col))

    def sideways_y(at, side):
        return remote(at, row, side, 5, 6, (along_y, col))

    def onward_x(at):
        return remote(at, along_y, 0, 7, 8, (along_x, col))

    def onward_y(at):
        return remote(at, along_x, 1, 7, 8, (along_y, col))

    def hand(at, quarter, side):
        return remote(at, quarter, side, 9 + quarter, 13 + quarter, (row, other))

    def hand_own():
        return pltpu.make_async_remote_copy(
            src_ref=held.at[col], dst_ref=held.at[col], send_sem=sems.at[17, 0],
            recv_sem=sems.at[18, 0], device_id=(row, other), device_id_type=MESH,
        )

    def keep(c):
        return pltpu.make_async_copy(held.at[c], out.at[c], stores.at[c])

    def both_ways(visit):
        for distance in range(1, chips):

            @pl.when(chip - distance >= 0)
            def _():
                visit(chip - distance, True)

            @pl.when(chip + distance <= last)
            def _():
                visit(chip + distance, False)

    load = pltpu.make_async_copy(mine, held.at[col], sems.at[19, 0])
    load.start()
    load.wait()

    def send_line(at, side, rising):
        if rising:

            @pl.when(chip < last)
            def _():
                up(at, side).start()

        else:

            @pl.when(chip > 0)
            def _():
                down(at, side).start()

    for side in range(2):
        send_line(chip, side, True)
        send_line(chip, side, False)
    hand_own().start()
    keep(col).start()

    def from_line(at, rising):
        for side in range(2):
            up(at, side).wait_recv()
            send_line(at, side, rising)
            sideways_x(at, side).start()
            sideways_y(at, side).start()
            hand(at, row, side).start()

    def from_sides(at, rising):
        for side in range(2):
            sideways_x(at, side).wait_recv()
            if side == 1:
                onward_y(at).start()
            sideways_y(at, side).wait_recv()
            if side == 0:
                onward_x(at).start()
            hand(at, along_x, side).start()
            hand(at, along_y, side).start()

    def from_across(at, rising):
        onward_x(at).wait_recv()
        hand(at, across, 0).start()
        onward_y(at).wait_recv()
        hand(at, across, 1).start()
        keep(2 * at + core).start()

    def from_other(at, rising):
        for quarter in range(4):
            for side in range(2):
                hand(at, quarter, side).wait_recv()
        keep(2 * at + 1 - core).start()

    both_ways(from_line)
    both_ways(from_sides)
    both_ways(from_across)
    hand_own().wait_recv()
    keep(other).start()
    both_ways(from_other)

    def drain_line(at, side, rising):
        if rising:

            @pl.when(chip < last)
            def _():
                up(at, side).wait_send()

        else:

            @pl.when(chip > 0)
            def _():
                down(at, side).wait_send()

    def drain(at, rising):
        for side in range(2):
            drain_line(at, side, rising)
            sideways_x(at, side).wait_send()
            sideways_y(at, side).wait_send()
            for quarter in range(4):
                hand(at, quarter, side).wait_send()
        onward_x(at).wait_send()
        onward_y(at).wait_send()

    both_ways(drain)
    for side in range(2):
        drain_line(chip, side, True)
        drain_line(chip, side, False)
    hand_own().wait_send()
    for c in range(2 * chips):
        keep(c).wait()


def gather_rows(mine, rows, cols):
    depth, wide = mine.shape
    piece = depth // 4
    if rows != 4 or piece % 16:
        return lax.all_gather(mine, "col", axis=0, tiled=True)
    shape = (cols, 4, piece, wide)
    out = pl.pallas_call(
        functools.partial(gather_kernel, cols // 2),
        out_shape=jax.ShapeDtypeStruct(shape, jnp.float32),
        in_specs=[ANYWHERE],
        out_specs=ANYWHERE,
        scratch_shapes=[
            pltpu.VMEM(shape, jnp.float32),
            pltpu.SemaphoreType.DMA((20, cols)),
            pltpu.SemaphoreType.DMA((cols,)),
        ],
        compiler_params=line_params(4),
        name="gather_rows",
    )(mine.reshape(4, piece, wide))
    return out.reshape(cols * depth, wide)


def lead_kernel(tile, flags, factor, listed, upper, coupling, high, low, lead, sep, *scratch):
    upper_high, upper_low, total = scratch
    wide = factor.shape[1]
    block = factor.shape[0] // listed.shape[1]

    for i in range(listed.shape[1]):
        at = pl.ds(i * block, block)
        sep[at, :] = factor[at, :] * listed[0, i : i + 1, :]

    def split(x):
        rounded = x.astype(jnp.bfloat16)
        return rounded, (x - rounded.astype(jnp.float32)).astype(jnp.bfloat16)

    def prepare(k, carry):
        at = pl.ds(pl.multiple_of(k * tile, tile), tile)
        upper_high[:, at], upper_low[:, at] = split(sep[:, at] * upper[:, at])
        return carry

    lax.fori_loop(0, wide // tile, prepare, 0)

    def column(m, carry):
        at = pl.ds(pl.multiple_of(m * tile, tile), tile)
        total[...] = -sep[:, at]

        def inner(k, carry):
            @pl.when(flags[k, m] != 0)
            def _():
                along = pl.ds(pl.multiple_of(k * tile, tile), tile)
                pair_high, pair_low = split(coupling[along, at])

                def times(left, right):
                    return jnp.dot(left[:, along], right, preferred_element_type=jnp.float32)

                term = times(upper_high, pair_low) + times(upper_low, pair_high)
                total[...] += term + times(upper_high, pair_high)

            return carry

        lax.fori_loop(0, wide // tile, inner, 0)
        lead[:, at] = total[...]
        high[at, :], low[at, :] = split(total[...].T)
        return carry

    lax.fori_loop(0, wide // tile, column, 0)


def lead_factors(factor, listed, upper, coupling, flags):
    tall, wide = factor.shape
    block = tall // listed.shape[0]
    step = 2 * block
    tile = wide // flags.shape[0]
    turned = pl.BlockSpec((wide, step), lambda i, f: (0, i))
    straight = pl.BlockSpec((step, wide), lambda i, f: (i, 0))
    return pl.pallas_call(
        functools.partial(lead_kernel, tile),
        out_shape=[jax.ShapeDtypeStruct((wide, tall), jnp.bfloat16)] * 2
        + [jax.ShapeDtypeStruct((tall, wide), jnp.float32)] * 2,
        grid_spec=pltpu.PrefetchScalarGridSpec(
            num_scalar_prefetch=1,
            grid=(tall // step,),
            in_specs=[
                straight,
                pl.BlockSpec((1, 2, wide), lambda i, f: (i, 0, 0)),
                pl.BlockSpec((1, wide), lambda i, f: (0, 0)),
                pl.BlockSpec((wide, wide), lambda i, f: (0, 0), pipeline_mode=pl.Buffered(1)),
            ],
            out_specs=[turned, turned, straight, straight],
            scratch_shapes=[
                pltpu.VMEM((step, wide), jnp.bfloat16),
                pltpu.VMEM((step, wide), jnp.bfloat16),
                pltpu.VMEM((step, tile), jnp.float32),
            ],
        ),
        compiler_params=pltpu.CompilerParams(vmem_limit_bytes=62 << 20),
        name="lead_factors",
    )(flags, factor, listed.reshape(-1, 2, wide), upper[None, :], coupling)


def shards(known_inverse, factor_sep, factor_pair, pivot_inverse, widths, parent_of, ancestors):
    col_index = lax.axis_index("col")
    row_index = lax.axis_index("row")
    rows = lax.axis_size("row")
    cols = lax.axis_size("col")
    chips = cols // 2
    chip, core = col_index // 2, col_index % 2
    sep_local = factor_sep.shape[0]
    pair_local = factor_pair.shape[0]
    wide_local = pivot_inverse.shape[1]
    column_owner, column_blocks, column_parent, column_upper = supernode_tables(
        widths, parent_of, ancestors
    )

    def rows_of(x, index, size):
        return lax.dynamic_slice_in_dim(x, index * size, size)

    def cols_of(x, index, size):
        return lax.dynamic_slice_in_dim(x, index * size, size, 1)

    blocks = sep_local // (NS // NBLK)
    listed = lax.dynamic_slice_in_dim(column_blocks, col_index * blocks, blocks, 1).T
    upper_cols = column_upper.astype(jnp.float32)
    owner_rows = rows_of(column_owner, col_index, pair_local)
    owner_wide = rows_of(column_owner, row_index, wide_local)
    parent_wide = rows_of(column_parent, row_index, wide_local)
    upper_wide = rows_of(column_upper, row_index, wide_local)
    coupling = jnp.where(
        (owner_rows[:, None] == column_parent[None, :]) & (~column_upper)[None, :], factor_pair, 0.0
    )
    matching = owner_rows[:, None] == owner_wide[None, :]
    match_pair = owner_rows[:, None] == parent_wide[None, :]

    coupling_all = gather_rows(coupling, rows, cols)

    straight = [
        (r * cols + 2 * z + q, z * cols + 2 * r + q)
        for r in range(rows)
        for z in range(chips)
        for q in range(2)
    ]
    crossed = [(source, target ^ 1) for source, target in straight]
    swapped = [(device, device ^ 1) for device in range(rows * cols)]

    def permute(x, order):
        return lax.ppermute(x, ("row", "col"), order)

    def ordered(mine, others):
        return jnp.where(
            core == 0, jnp.concatenate([mine, others]), jnp.concatenate([others, mine])
        )

    upper_pivot = jnp.where(matching & upper_wide[None, :], pivot_inverse, 0.0)
    pivot_tile = ordered(
        permute(cols_of(upper_pivot, core, pair_local), straight),
        permute(cols_of(upper_pivot, 1 - core, pair_local), crossed),
    )
    pivot_coupled = plain_dot(pivot_tile, coupling)

    nodes = jnp.arange(NSUP, dtype=jnp.int32)
    tiles = WTOT // 256
    holds = jnp.any(column_owner.reshape(tiles, 256, 1) == nodes, axis=1)
    wants = jnp.any(column_parent.reshape(tiles, 256, 1) == nodes, axis=1)
    flags = jnp.any(holds[:, None, :] & wants[None, :, :], axis=2).astype(jnp.int32)
    high, low, lead, sep_factor = lead_factors(
        factor_sep, listed, upper_cols, coupling_all, flags
    )
    panel, product = panel_reduce(
        high,
        low,
        known_inverse,
        sep_factor,
        lead,
        pivot_coupled,
        upper_wide.astype(jnp.float32),
        chips,
    )
    tile = block_reduce(product, chips)

    dealt_tile = permute(tile, straight)
    pair_tile = jnp.where(
        rows_of(column_owner, 2 * row_index + core, pair_local)[:, None]
        == rows_of(column_parent, chip, wide_local)[None, :],
        -tile,
        0.0,
    )
    pair_cols = ordered(
        cols_of(pair_tile, core, pair_local),
        permute(cols_of(pair_tile, 1 - core, pair_local), swapped),
    )
    below = first_dot(pair_cols, rows_of(coupling_all, row_index, wide_local))
    below = plane_reduce(below, rows)

    own_block = jnp.where(
        matching, pivot_inverse - dealt_tile - jnp.where(upper_wide[None, :], 0.0, below), 0.0
    )
    return panel, own_block + jnp.where(match_pair, -dealt_tile, 0.0)


def solution(mesh):
    if mesh.shape["col"] != 2 * mesh.shape["row"]:
        raise ValueError("unsupported mesh")
    in_specs = (P("col", "row"), P("col", None), P("col", None), P("col", "row"), P(), P(), P())
    out_specs = (P("col", "row"), P("col", "row"))
    return jax.shard_map(shards, mesh=mesh, in_specs=in_specs, out_specs=out_specs, check_vma=False)
```
